32 devices in a mesh: dp: 8 (over z, y), mp: 4 (over x, core).
Axes of the slice: x: 2, y: 2, z: 4, core: 2. Of those that a mesh axis runs over, the one named last changes fastest.
Arguments:
- queries: bfloat16 [128, 8192], P('dp', 'mp'), may hold values from -8 to 8
- incoming_key: bfloat16 [128, 1024], P('dp', 'mp'), may hold values from -4 to 4
- incoming_value: bfloat16 [128, 1024], P('dp', 'mp'), may hold values from -4 to 4
- key_cache: bfloat16 [256, 256, 1024], P('dp', None, 'mp'), may hold values from -8 to 8
- cached_values: bfloat16 [256, 256, 1024], P('dp', None, 'mp'), may hold values from -4 to 4
- task_key_scale: bfloat16 [256, 1024], P(None, 'mp'), may hold values from 0.099609375 to 1.8984375
- task_value_scale: bfloat16 [256, 1024], P(None, 'mp'), may hold values from 0.099609375 to 1.8984375
- out_weight: bfloat16 [8192, 8192], P('mp', 'dp'), may hold values from -0.0625 to 0.0625
- task_id: int32 [128], P('dp'), may hold values from 0 to 255, as said below
- cached_length: int32 [128], P('dp'), may hold values from 1 to 256, as said below
- task_owner: int32 [256], replicated, may hold values from 0 to 7, as said below
- cache_slot: int32 [128], P('dp'), may hold values from 0 to 31, as said below
Outputs:
- layer_out: bfloat16 [128, 8192], P('dp', 'mp')
The draws below stay inside these ranges and needn't reach their ends.
Inputs may be any that keep to these rules, and one draw needn't show every extreme that they name: `task_owner`: every dp index owns the same number of tasks. `task_id`: among the 16 requests of one dp index at most 4 have tasks of one owner; in every draw one owner gets exactly 4 from every dp index. `cache_slot`: requests of one owner have distinct slots; one owner uses all 32. `cached_length`: every dp index has a request with 256 cached positions.
All inputs are finite; a program needn't handle non-finite values.
Results may differ from the reference program's by a relative error of at most 0.0073.
Values may be sent and summed in bfloat16 or wider, within the bound.
A program may use at most 128 MiB of HBM per device.

```python
import math
import jax
import jax.numpy as jnp
from jax import lax

D = 8192
KEY_VALUE_HEADS = 8
HEAD_SIZE = 128
QUERY_HEADS = 64
TASK_TOTAL = 256
REQUESTS_PER_DP = 16
MAX_POSITIONS = 256
QUERY_PER_KV = 8
REQUEST_TOTAL = 128
CAP = 4
OWN_CAP = 32
CACHE_ROWS = 256
N_DP = 8


def routing(key):
    shuffle = jax.random.permutation(jax.random.fold_in(key, 11), TASK_TOTAL)
    task_owner = (shuffle % N_DP).astype(jnp.int32)
    hot_owner = jax.random.randint(jax.random.fold_in(key, 12), (), 0, N_DP)
    position = jnp.arange(REQUESTS_PER_DP)
    rotation = jax.random.randint(jax.random.fold_in(key, 13), (N_DP, 1), 0, N_DP - 1)
    others = (hot_owner + 1 + (position[None, :] - CAP + rotation) % (N_DP - 1)) % N_DP
    owners_block = jnp.where(position[None, :] < CAP, hot_owner, others)
    block_keys = jax.random.split(jax.random.fold_in(key, 14), N_DP)
    orders = jax.vmap(lambda one_key: jax.random.permutation(one_key, REQUESTS_PER_DP))(block_keys)
    owners = jnp.take_along_axis(owners_block, orders, axis=1).reshape(REQUEST_TOTAL)
    within = jax.random.randint(jax.random.fold_in(key, 15), (REQUEST_TOTAL,), 0, TASK_TOTAL // N_DP)
    inverse = jnp.argsort(shuffle)
    task_id = inverse[owners + N_DP * within].astype(jnp.int32)
    mixing = jax.random.permutation(jax.random.fold_in(key, 16), REQUEST_TOTAL)
    ranking = jnp.argsort(owners * REQUEST_TOTAL + mixing)
    sorted_owner = owners[ranking]
    counts = jnp.sum((sorted_owner[:, None] == jnp.arange(N_DP)[None, :]).astype(jnp.int32), axis=0)
    starts = jnp.cumsum(counts) - counts
    rank_sorted = jnp.arange(REQUEST_TOTAL) - starts[sorted_owner]
    cache_slot = jnp.zeros((REQUEST_TOTAL,), jnp.int32).at[ranking].set(rank_sorted.astype(jnp.int32))
    return (task_owner, task_id, cache_slot)


def draw_task_owner(key, part):
    return routing(key)[0]


def draw_task_id(key, part):
    return routing(key)[1]


def draw_cache_slot(key, part):
    return routing(key)[2]


def draw_cached_length(key, part):
    lengths = jax.random.randint(jax.random.fold_in(key, 21), (N_DP, REQUESTS_PER_DP), 1, MAX_POSITIONS + 1)
    longest = jax.random.randint(jax.random.fold_in(key, 22), (N_DP, 1), 0, REQUESTS_PER_DP)
    lengths = jnp.where(jnp.arange(REQUESTS_PER_DP)[None, :] == longest, MAX_POSITIONS, lengths)
    return lengths.reshape(REQUEST_TOTAL).astype(jnp.int32)


def draw_queries(key, part):
    random_noise = jax.random.normal(jax.random.fold_in(key, 32), (REQUEST_TOTAL, QUERY_HEADS * HEAD_SIZE), jnp.float32)
    value_rows = jnp.clip(2.0 * random_noise, -6.0, 6.0)
    return value_rows.astype(jnp.bfloat16)


def draw_key_cache(key, part):
    random_noise = jax.random.normal(jax.random.fold_in(key, 33), (CACHE_ROWS, MAX_POSITIONS, KEY_VALUE_HEADS * HEAD_SIZE), jnp.float32)
    value_rows = jnp.clip(random_noise, -4.0, 4.0)
    return value_rows.astype(jnp.bfloat16)


def block_levels(key, dims, cuts, least, top_value):
    loudness, own = 1.0, jax.random.fold_in(key, 6)
    for dim, shards_of in cuts:
        draws = jnp.exp(jax.random.uniform(jax.random.fold_in(own, dim), (shards_of,), jnp.float32, least / len(cuts), top_value / len(cuts)))
        loudness = loudness * jnp.repeat(draws, dims[dim] // shards_of).reshape([-1 if axis == dim else 1 for axis in range(len(dims))])
    return loudness


def normal_values(stream_key, shape, scale, most, pieces=(), kind=jnp.bfloat16):
    values = jax.random.normal(stream_key, shape, jnp.float32) * scale
    if len(pieces) > 0:
        values = block_levels(stream_key, shape, pieces, -0.22, 0.18) * values
    return jnp.clip(values, min=-most, max=most).astype(kind)


def setup_inputs(seed: int = 0) -> dict:
    streams_of = jax.random.split(jax.random.key(seed), 13)
    return {
        "queries": draw_queries(jax.random.fold_in(streams_of[12], 71), 0),
        "incoming_key": normal_values(streams_of[1], (REQUEST_TOTAL, KEY_VALUE_HEADS * HEAD_SIZE), 1.0, 4.0, ((0, 8), (1, 4))),
        "incoming_value": normal_values(streams_of[2], (REQUEST_TOTAL, KEY_VALUE_HEADS * HEAD_SIZE), 1.0, 4.0, ((0, 8), (1, 4))),
        "key_cache": draw_key_cache(jax.random.fold_in(streams_of[12], 71), 0),
        "cached_values": normal_values(streams_of[4], (CACHE_ROWS, MAX_POSITIONS, KEY_VALUE_HEADS * HEAD_SIZE), 1.0, 4.0, ((0, 8), (2, 4))),
        "task_key_scale": jnp.clip(1.0 + 0.18 * jax.random.normal(streams_of[5], (TASK_TOTAL, KEY_VALUE_HEADS * HEAD_SIZE), jnp.float32), 0.099609375, 1.8984375).astype(jnp.bfloat16),
        "task_value_scale": jnp.clip(1.0 + 0.18 * jax.random.normal(streams_of[6], (TASK_TOTAL, KEY_VALUE_HEADS * HEAD_SIZE), jnp.float32), 0.099609375, 1.8984375).astype(jnp.bfloat16),
        "out_weight": normal_values(streams_of[7], (QUERY_HEADS * HEAD_SIZE, D), (QUERY_HEADS * HEAD_SIZE) ** -0.5, 0.0625, ((0, 4), (1, 8))),
        "task_id": draw_task_id(jax.random.fold_in(streams_of[12], 71), 0),
        "cached_length": draw_cached_length(jax.random.fold_in(streams_of[12], 71), 0),
        "task_owner": draw_task_owner(jax.random.fold_in(streams_of[12], 71), 0),
        "cache_slot": draw_cache_slot(jax.random.fold_in(streams_of[12], 71), 0),
    }


masked_score = -1e+30

def lowered_program(value_rows):
    return lax.optimization_barrier(value_rows.astype(jnp.bfloat16))

def attend(queries, fresh_key_rows, fresh_value_rows, stored_key_rows, stored_value_rows, lengths):
    entry_count = queries.shape[0]
    inv_root = 1.0 / math.sqrt(HEAD_SIZE)
    query_head_rows = queries.astype(jnp.float32).reshape(entry_count, KEY_VALUE_HEADS, QUERY_PER_KV, HEAD_SIZE)
    previous_keys = stored_key_rows.astype(jnp.float32).reshape(entry_count, MAX_POSITIONS, KEY_VALUE_HEADS, HEAD_SIZE)
    previous_values = stored_value_rows.astype(jnp.float32).reshape(entry_count, MAX_POSITIONS, KEY_VALUE_HEADS, HEAD_SIZE)
    incoming_keys = fresh_key_rows.astype(jnp.float32).reshape(entry_count, KEY_VALUE_HEADS, HEAD_SIZE)
    incoming_values = fresh_value_rows.astype(jnp.float32).reshape(entry_count, KEY_VALUE_HEADS, HEAD_SIZE)
    scores = jnp.einsum('ngqd,njgd->ngqj', query_head_rows, previous_keys, precision=lax.Precision.HIGHEST) * inv_root
    own_score = jnp.einsum('ngqd,ngd->ngq', query_head_rows, incoming_keys, precision=lax.Precision.HIGHEST) * inv_root
    visible = jnp.arange(MAX_POSITIONS)[None, None, None, :] < lengths[:, None, None, None]
    scores = jnp.where(visible, scores, masked_score)
    top_score = jnp.maximum(lax.optimization_barrier(jnp.max(scores, axis=3)), own_score)
    weights = jnp.where(visible, jnp.exp(scores - top_score[..., None]), 0.0)
    own_weight = jnp.exp(own_score - top_score)
    weight_sum = lax.optimization_barrier(jnp.sum(weights, axis=3)) + own_weight
    blended = jnp.einsum('ngqj,njgd->ngqd', lowered_program(weights).astype(jnp.float32), previous_values, precision=lax.Precision.HIGHEST)
    blended = blended + lowered_program(own_weight).astype(jnp.float32)[..., None] * incoming_values[:, :, None, :]
    return (blended / weight_sum[..., None]).astype(jnp.bfloat16).reshape(entry_count, QUERY_HEADS * HEAD_SIZE)

def reference(queries, incoming_key, incoming_value, key_cache, cached_values, task_key_scale, task_value_scale, out_weight, task_id, cached_length, task_owner, cache_slot):
    owner_of = jnp.take(task_owner, task_id).astype(jnp.int32)
    owner_row_index = (owner_of * OWN_CAP + cache_slot).astype(jnp.int32)
    key_factor = jnp.take(task_key_scale, task_id, axis=0).astype(jnp.float32)
    value_factor = jnp.take(task_value_scale, task_id, axis=0).astype(jnp.float32)
    scaled_rows = lowered_program((queries.astype(jnp.float32).reshape(REQUEST_TOTAL, KEY_VALUE_HEADS, QUERY_PER_KV, HEAD_SIZE) * key_factor.reshape(REQUEST_TOTAL, KEY_VALUE_HEADS, 1, HEAD_SIZE)).reshape(REQUEST_TOTAL, QUERY_HEADS * HEAD_SIZE))

    def block_kernel(members):
        block_queries, block_keys, block_values, block_rows, block_lengths = members
        stored_key_rows = jnp.take(key_cache, block_rows, axis=0)
        stored_value_rows = jnp.take(cached_values, block_rows, axis=0)
        return attend(block_queries, block_keys, block_values, stored_key_rows, stored_value_rows, block_lengths)
    attention_output = lax.map(block_kernel, (scaled_rows.reshape(N_DP, REQUESTS_PER_DP, QUERY_HEADS * HEAD_SIZE), incoming_key.reshape(N_DP, REQUESTS_PER_DP, KEY_VALUE_HEADS * HEAD_SIZE), incoming_value.reshape(N_DP, REQUESTS_PER_DP, KEY_VALUE_HEADS * HEAD_SIZE), owner_row_index.reshape(N_DP, REQUESTS_PER_DP), cached_length.reshape(N_DP, REQUESTS_PER_DP)))
    attention_output = attention_output.reshape(REQUEST_TOTAL, QUERY_HEADS * HEAD_SIZE)
    context_rows = lowered_program((attention_output.astype(jnp.float32).reshape(REQUEST_TOTAL, KEY_VALUE_HEADS, QUERY_PER_KV, HEAD_SIZE) * value_factor.reshape(REQUEST_TOTAL, KEY_VALUE_HEADS, 1, HEAD_SIZE)).reshape(REQUEST_TOTAL, QUERY_HEADS * HEAD_SIZE))
    return jnp.dot(context_rows, out_weight, preferred_element_type=jnp.float32).astype(jnp.bfloat16)
```

```python
import math

import jax
import jax.numpy as jnp
from jax import lax
from jax.sharding import PartitionSpec as P

KEY_VALUE_HEADS = 8
HEAD_SIZE = 128
QUERY_HEADS = 64
MAX_POSITIONS = 256


masked_score = -1e30


def attend(queries, fresh_key_rows, fresh_value_rows, stored_key_rows, stored_value_rows, lengths):
    entry_count = queries.shape[0]
    kv_heads = fresh_key_rows.shape[1] // HEAD_SIZE
    group_width = QUERY_HEADS // KEY_VALUE_HEADS
    inv_root = 1.0 / math.sqrt(HEAD_SIZE)
    query_head_rows = queries.reshape(entry_count, kv_heads, group_width, HEAD_SIZE)
    previous_keys = stored_key_rows.reshape(entry_count, MAX_POSITIONS, kv_heads, HEAD_SIZE)
    previous_values = stored_value_rows.reshape(entry_count, MAX_POSITIONS, kv_heads, HEAD_SIZE)
    incoming_keys = fresh_key_rows.reshape(entry_count, kv_heads, HEAD_SIZE)
    incoming_values = fresh_value_rows.reshape(entry_count, kv_heads, HEAD_SIZE)
    scores = (
        jnp.einsum(
            "ngqd,njgd->ngqj", query_head_rows, previous_keys, preferred_element_type=jnp.float32
        )
        * inv_root
    )
    own_score = (
        jnp.einsum(
            "ngqd,ngd->ngq", query_head_rows, incoming_keys, preferred_element_type=jnp.float32
        )
        * inv_root
    )
    visible = (
        lax.broadcasted_iota(jnp.int32, (entry_count, 1, 1, MAX_POSITIONS), 3)
        < lengths[:, None, None, None]
    )
    scores = jnp.where(visible, scores, masked_score)
    top_score = jnp.maximum(jnp.max(scores, axis=3), own_score)
    weights = jnp.where(visible, jnp.exp(scores - top_score[..., None]), 0.0)
    own_weight = jnp.exp(own_score - top_score)
    weight_sum = jnp.sum(weights, axis=3) + own_weight
    blended = jnp.einsum(
        "ngqj,njgd->ngqd",
        weights.astype(jnp.bfloat16),
        previous_values,
        preferred_element_type=jnp.float32,
    )
    blended = (
        blended
        + own_weight.astype(jnp.bfloat16).astype(jnp.float32)[..., None]
        * incoming_values.astype(jnp.float32)[:, :, None, :]
    )
    return (
        (blended / weight_sum[..., None])
        .astype(jnp.bfloat16)
        .reshape(entry_count, kv_heads * group_width * HEAD_SIZE)
    )


def on_device(
    queries,
    incoming_key,
    incoming_value,
    key_cache,
    cached_values,
    task_key_scale,
    task_value_scale,
    out_weight,
    task_id,
    cached_length,
    task_owner,
    cache_slot,
):
    row_count = queries.shape[0]
    task_count = task_key_scale.shape[0]
    kv_width = incoming_key.shape[1]
    kv_heads = kv_width // HEAD_SIZE
    group_width = QUERY_HEADS // KEY_VALUE_HEADS
    owner_count = lax.axis_size("dp")
    capacity = 2 * row_count // owner_count
    picked = task_id[:, None] == lax.broadcasted_iota(jnp.int32, (row_count, task_count), 1)
    owner_of = jnp.sum(jnp.where(picked, task_owner[None, :], 0), axis=1)
    selector = picked.astype(jnp.bfloat16)
    key_factor = jnp.dot(selector, task_key_scale, preferred_element_type=jnp.float32)
    value_factor = jnp.dot(selector, task_value_scale, preferred_element_type=jnp.float32)
    scaled_rows = (
        (
            queries.astype(jnp.float32).reshape(row_count, kv_heads, group_width, HEAD_SIZE)
            * key_factor.reshape(row_count, kv_heads, 1, HEAD_SIZE)
        )
        .astype(jnp.bfloat16)
        .reshape(row_count, kv_heads * group_width * HEAD_SIZE)
    )
    head_width = scaled_rows.shape[1]
    earlier = lax.broadcasted_iota(jnp.int32, (row_count, row_count), 1) < lax.broadcasted_iota(
        jnp.int32, (row_count, row_count), 0
    )
    same_owner = owner_of[:, None] == owner_of[None, :]
    rank_in = jnp.sum(jnp.where(earlier & same_owner, 1, 0), axis=1)
    position = owner_of * capacity + rank_in
    slot_total = owner_count * capacity
    placing = position[None, :] == lax.broadcasted_iota(jnp.int32, (slot_total, row_count), 0)
    packer = placing.astype(jnp.bfloat16)
    unpacker = (
        position[:, None] == lax.broadcasted_iota(jnp.int32, (row_count, slot_total), 1)
    ).astype(jnp.bfloat16)

    def pack_rows(value_rows):
        packed = jnp.dot(packer, value_rows, preferred_element_type=jnp.float32).astype(
            jnp.bfloat16
        )
        return packed.reshape(owner_count, capacity, value_rows.shape[1])

    def pack_ints(value_rows):
        return (
            jnp.sum(jnp.where(placing, value_rows[None, :] + 1, 0), axis=1).reshape(
                owner_count, capacity
            )
            - 1
        )

    got_queries = lax.all_to_all(
        pack_rows(scaled_rows), "dp", split_axis=0, concat_axis=0, tiled=True
    )
    got_keys = lax.all_to_all(
        pack_rows(incoming_key), "dp", split_axis=0, concat_axis=0, tiled=True
    )
    got_values = lax.all_to_all(
        pack_rows(incoming_value), "dp", split_axis=0, concat_axis=0, tiled=True
    )
    slot_ids = lax.all_to_all(pack_ints(cache_slot), "dp", split_axis=0, concat_axis=0, tiled=True)
    got_lengths = lax.all_to_all(
        pack_ints(cached_length), "dp", split_axis=0, concat_axis=0, tiled=True
    )
    sources = slot_ids.shape[0]
    per_source = slot_ids.shape[1]
    item_total = sources * per_source
    flat_slots = jnp.maximum(slot_ids.reshape(item_total), 0)
    stored_key_rows = jnp.take(key_cache, flat_slots, axis=0)
    stored_value_rows = jnp.take(cached_values, flat_slots, axis=0)
    result = attend(
        got_queries.reshape(item_total, head_width),
        got_keys.reshape(item_total, kv_width),
        got_values.reshape(item_total, kv_width),
        stored_key_rows,
        stored_value_rows,
        got_lengths.reshape(item_total),
    )
    answered = result.reshape(sources, per_source, head_width)
    returned = lax.all_to_all(answered, "dp", split_axis=0, concat_axis=0, tiled=True)
    attention_output = jnp.dot(
        unpacker, returned.reshape(slot_total, head_width), preferred_element_type=jnp.float32
    ).astype(jnp.bfloat16)
    context_rows = (
        (
            attention_output.astype(jnp.float32).reshape(
                row_count, kv_heads, group_width, HEAD_SIZE
            )
            * value_factor.reshape(row_count, kv_heads, 1, HEAD_SIZE)
        )
        .astype(jnp.bfloat16)
        .reshape(row_count, head_width)
    )
    all_rows = lax.all_gather(context_rows, "dp", axis=0, tiled=True)
    partial_value = jnp.dot(all_rows, out_weight, preferred_element_type=jnp.float32).astype(
        jnp.bfloat16
    )
    own_rows = lax.all_to_all(partial_value, "dp", split_axis=0, concat_axis=1, tiled=True)
    return lax.psum_scatter(
        own_rows.astype(jnp.float32), "mp", scatter_dimension=1, tiled=True
    ).astype(jnp.bfloat16)


def solution(mesh):
    placed = (
        P("dp", "mp"),
        P("dp", "mp"),
        P("dp", "mp"),
        P("dp", None, "mp"),
        P("dp", None, "mp"),
        P(None, "mp"),
        P(None, "mp"),
        P("mp", "dp"),
        P("dp"),
        P("dp"),
        P(),
        P("dp"),
    )
    return jax.shard_map(
        on_device, mesh=mesh, in_specs=placed, out_specs=P("dp", "mp"), check_vma=False
    )
```

```python
import functools
import math

import jax
import jax.numpy as jnp
from jax import lax
from jax.experimental import pallas as pl
from jax.experimental.pallas import tpu as pltpu
from jax.sharding import PartitionSpec as P

KEY_VALUE_HEADS = 8
HEAD_SIZE = 128
QUERY_HEADS = 64
GROUP = QUERY_HEADS // KEY_VALUE_HEADS
META = 128
FIRST = 16
MESH = pl.DeviceIdType.MESH

masked_score = -1e30
f32 = jnp.float32
bf16 = jnp.bfloat16


def iota(shape, dim):
    return lax.broadcasted_iota(jnp.int32, shape, dim)


def to_column(row):
    n = row.shape[1]
    eye = iota((n, n), 0) == iota((n, n), 1)
    return jnp.sum(jnp.where(eye, row, 0.0), axis=1, keepdims=True)


def to_row(column):
    n = column.shape[0]
    eye = iota((n, n), 0) == iota((n, n), 1)
    return jnp.sum(jnp.where(eye, column, 0.0), axis=0, keepdims=True)


def dot(a, b):
    return jnp.dot(a, b, preferred_element_type=f32)


def layer_kernel(
    dp,
    mp,
    query_ref,
    new_key_ref,
    new_value_ref,
    key_scale_ref,
    value_scale_ref,
    task_ref,
    length_ref,
    slot_ref,
    owner_ref,
    key_hbm,
    value_hbm,
    weight_hbm,
    out_ref,
    keys,
    values,
    weight,
    rows_f32,
    send_rows,
    recv_rows,
    slot_query,
    slot_small,
    slot_length,
    slot_context,
    context,
    selector,
    send_part,
    recv_part,
    local_sem,
    send_sem,
    recv_sem,
):
    me = lax.axis_index("dp")
    part = lax.axis_index("mp")
    rows, query_width = query_ref.shape
    kv_width = new_key_ref.shape[1]
    kv_heads = kv_width // HEAD_SIZE
    heads = kv_heads * GROUP
    task_total = key_scale_ref.shape[0]
    slots, positions, _ = keys.shape
    capacity = send_rows.shape[1]
    items = dp * capacity
    columns = weight.shape[1]
    blocks = dp // mp
    meta_at = query_width + 2 * kv_width

    total = dp * mp
    here = me * mp + part
    barrier = pltpu.get_barrier_semaphore()

    def greet(k, carry):
        other = lax.rem(here + k, total)
        pl.semaphore_signal(
            barrier,
            inc=1,
            device_id=(other // mp, lax.rem(other, mp)),
            device_id_type=MESH,
        )
        return carry

    lax.fori_loop(1, total, greet, 0)

    fetches = [
        pltpu.make_async_copy(key_hbm, keys, local_sem.at[0]),
        pltpu.make_async_copy(value_hbm, values, local_sem.at[1]),
        pltpu.make_async_copy(weight_hbm, weight, local_sem.at[2]),
    ]
    for fetch in fetches:
        fetch.start()

    task_column = to_column(task_ref[...].astype(f32))
    length_column = to_column(length_ref[...].astype(f32))
    slot_column = to_column(slot_ref[...].astype(f32))
    picked = task_column == iota((rows, task_total), 1).astype(f32)
    owner_column = jnp.sum(
        jnp.where(picked, owner_ref[...].astype(f32), 0.0), axis=1, keepdims=True
    )
    owner_row = to_row(owner_column)
    earlier = iota((rows, rows), 1) < iota((rows, rows), 0)
    rank = jnp.sum(
        jnp.where(earlier & (owner_column == owner_row), 1.0, 0.0), axis=1, keepdims=True
    )
    position_row = to_row(owner_column * capacity + rank)
    packer = jnp.where(position_row == iota((items, rows), 0).astype(f32), 1.0, 0.0).astype(bf16)
    key_factor = dot(jnp.where(picked, 1.0, 0.0).astype(bf16), key_scale_ref[...])
    for h in range(heads):
        g = h // GROUP
        lanes = slice(h * HEAD_SIZE, (h + 1) * HEAD_SIZE)
        scaled = (
            query_ref[:, lanes].astype(f32) * key_factor[:, g * HEAD_SIZE : (g + 1) * HEAD_SIZE]
        ).astype(bf16)
        rows_f32[:, lanes] = dot(packer, scaled)
    rows_f32[:, query_width : query_width + kv_width] = dot(packer, new_key_ref[...])
    rows_f32[:, query_width + kv_width : meta_at] = dot(packer, new_value_ref[...])
    lane = iota((rows, META), 1)
    line = iota((rows, META), 0)
    task_high = jnp.floor(task_column * (1.0 / 128.0))
    task_low = task_column - task_high * 128.0
    facts = (
        jnp.where(lane == 0, slot_column + 1.0, 0.0)
        + jnp.where(lane == 1, length_column, 0.0)
        + jnp.where(lane == 2, task_high, 0.0)
        + jnp.where(lane == 3, task_low, 0.0)
    )
    shared = jnp.sum(
        jnp.where(lane == FIRST + line, owner_column, 0.0)
        + jnp.where(lane == FIRST + rows + line, slot_column, 0.0),
        axis=0,
        keepdims=True,
    )
    rows_f32[:, meta_at:] = dot(packer, facts.astype(bf16)) + shared
    for d in range(dp):
        send_rows[d] = rows_f32[d * capacity : (d + 1) * capacity, :].astype(bf16)

    pl.semaphore_wait(barrier, total - 1)

    def request_copy(k):
        return pltpu.make_async_remote_copy(
            src_ref=send_rows.at[lax.rem(me + k, dp)],
            dst_ref=recv_rows.at[me],
            send_sem=send_sem.at[0, k],
            recv_sem=recv_sem.at[0, k],
            device_id=(lax.rem(me + k, dp), part),
            device_id_type=MESH,
        )

    def request_arrival(k):
        return pltpu.make_async_remote_copy(
            src_ref=send_rows.at[0],
            dst_ref=recv_rows.at[lax.rem(me + dp - k, dp)],
            send_sem=send_sem.at[0, k],
            recv_sem=recv_sem.at[0, k],
            device_id=(lax.rem(me + k, dp), part),
            device_id_type=MESH,
        )

    for k in range(1, dp):
        request_copy(k).start()
    recv_rows[me] = send_rows[me]
    slot_query[...] = jnp.zeros_like(slot_query)
    for k in range(1, dp):
        request_arrival(k).wait_recv()

    for s in range(dp):
        rows_f32[s * capacity : (s + 1) * capacity, :] = recv_rows[s].astype(f32)
    facts_in = rows_f32[:, meta_at:]
    placing_row = to_row(facts_in[:, 0:1])
    placer = jnp.where(
        placing_row == iota((slots, items), 0).astype(f32) + 1.0, 1.0, 0.0
    ).astype(bf16)
    for h in range(heads):
        g = h // GROUP
        slot_query[:, h, g * HEAD_SIZE : (g + 1) * HEAD_SIZE] = dot(
            placer, rows_f32[:, h * HEAD_SIZE : (h + 1) * HEAD_SIZE].astype(bf16)
        )
    slot_small[0] = dot(placer, rows_f32[:, query_width : query_width + kv_width].astype(bf16))
    slot_small[1] = dot(placer, rows_f32[:, query_width + kv_width : meta_at].astype(bf16))
    slot_facts = dot(placer, facts_in.astype(bf16))
    slot_task = slot_facts[:, 2:3] * 128.0 + slot_facts[:, 3:4]
    slot_small[2] = dot(
        jnp.where(slot_task == iota((slots, task_total), 1).astype(f32), 1.0, 0.0).astype(bf16),
        value_scale_ref[...],
    )
    slot_length[...] = jnp.broadcast_to(slot_facts[:, 1:2], (slots, positions))

    fetches[0].wait()
    fetches[1].wait()
    inv_root = 1.0 / math.sqrt(HEAD_SIZE)
    key_line = iota((heads, positions), 1).astype(f32)

    def attend(s, carry):
        query = slot_query[s]
        one = pl.ds(s, 1)
        fresh_key = slot_small[0, one, :]
        fresh_value = slot_small[1, one, :]
        value_factor = slot_small[2, one, :]
        length = slot_length[one, :]
        scores = (
            lax.dot_general(
                query.astype(bf16), keys[s], (((1,), (1,)), ((), ())), preferred_element_type=f32
            )
            * inv_root
        )
        own = jnp.sum(query * fresh_key, axis=1, keepdims=True) * inv_root
        visible = key_line < length
        scores = jnp.where(visible, scores, masked_score)
        top = jnp.maximum(jnp.max(scores, axis=1, keepdims=True), own)
        weights = jnp.where(visible, jnp.exp(scores - top), 0.0)
        own_weight = jnp.exp(own - top)
        weight_sum = jnp.sum(weights, axis=1, keepdims=True) + own_weight
        blended = dot(weights.astype(bf16), values[s])
        blended = blended + own_weight.astype(bf16).astype(f32) * fresh_value
        attended = (blended / weight_sum).astype(bf16).astype(f32) * value_factor
        for g in range(kv_heads):
            slot_context[s, g * GROUP : (g + 1) * GROUP, :] = attended[
                g * GROUP : (g + 1) * GROUP, g * HEAD_SIZE : (g + 1) * HEAD_SIZE
            ]
        return carry

    lax.fori_loop(0, slots, attend, 0, unroll=4)
    for h in range(heads):
        context[me, :, h * HEAD_SIZE : (h + 1) * HEAD_SIZE] = slot_context[:, h, :].astype(bf16)

    def context_copy(k, source):
        return pltpu.make_async_remote_copy(
            src_ref=context.at[source],
            dst_ref=context.at[source],
            send_sem=send_sem.at[1, k],
            recv_sem=recv_sem.at[1, k],
            device_id=(lax.rem(me + k, dp), part),
            device_id_type=MESH,
        )

    for k in range(1, dp):
        context_copy(k, me).start()

    lane_r = iota((rows, META), 1)
    line_r = iota((rows, META), 0)
    for s in range(dp):
        fact_row = rows_f32[s * capacity : s * capacity + 1, meta_at:]
        owner_in = jnp.sum(
            jnp.where(lane_r == FIRST + line_r, fact_row, 0.0), axis=1, keepdims=True
        )
        slot_in = jnp.sum(
            jnp.where(lane_r == FIRST + rows + line_r, fact_row, 0.0), axis=1, keepdims=True
        )
        selector[s * rows : (s + 1) * rows, :] = jnp.where(
            owner_in * slots + slot_in == iota((rows, dp * slots), 1).astype(f32), 1.0, 0.0
        ).astype(bf16)
    fetches[2].wait()
    for k in range(1, dp):
        context_copy(k, lax.rem(me + dp - k, dp)).wait_recv()

    arranged = dot(selector[...], context[...].reshape(dp * slots, query_width)).astype(bf16)
    send_part[...] = dot(arranged, weight[...]).astype(bf16).reshape(dp, rows, columns)

    target_part = me // blocks
    place = lax.rem(me, blocks) * mp + part

    def part_copy(k):
        target = lax.rem(me + k, dp)
        return pltpu.make_async_remote_copy(
            src_ref=send_part.at[target],
            dst_ref=recv_part.at[place],
            send_sem=send_sem.at[2, k],
            recv_sem=recv_sem.at[2, place],
            device_id=(target, target_part),
            device_id_type=MESH,
        )

    def part_arrival(j):
        return pltpu.make_async_remote_copy(
            src_ref=send_part.at[0],
            dst_ref=recv_part.at[j],
            send_sem=send_sem.at[2, 0],
            recv_sem=recv_sem.at[2, j],
            device_id=(me, part),
            device_id_type=MESH,
        )

    for k in range(1, dp):
        part_copy(k).start()

    @pl.when(target_part != part)
    def _():
        part_copy(0).start()

    @pl.when(target_part == part)
    def _():
        recv_part[place] = send_part[me]

    for j in range(dp):
        own_block = (part * blocks + j // mp == me) & (part == j % mp)

        @pl.when(jnp.logical_not(own_block))
        def _():
            part_arrival(j).wait_recv()

    for e in range(blocks):
        summed = recv_part[e * mp].astype(f32)
        for j in range(1, mp):
            summed = summed + recv_part[e * mp + j].astype(f32)
        out_ref[:, e * columns : (e + 1) * columns] = summed.astype(bf16)

    for k in range(1, dp):
        request_copy(k).wait_send()
        context_copy(k, me).wait_send()
        part_copy(k).wait_send()

    @pl.when(target_part != part)
    def _():
        part_copy(0).wait_send()


def on_device(
    dp,
    mp,
    queries,
    incoming_key,
    incoming_value,
    key_cache,
    cached_values,
    task_key_scale,
    task_value_scale,
    out_weight,
    task_id,
    cached_length,
    task_owner,
    cache_slot,
):
    rows, query_width = queries.shape
    kv_width = incoming_key.shape[1]
    slots = key_cache.shape[0]
    capacity = 2 * rows // dp
    items = dp * capacity
    columns = out_weight.shape[1]
    row_width = query_width + 2 * kv_width + META
    heads = query_width // HEAD_SIZE
    vmem = pl.BlockSpec(memory_space=pltpu.VMEM)
    away = pl.BlockSpec(memory_space=pl.ANY)
    return pl.pallas_call(
        functools.partial(layer_kernel, dp, mp),
        out_shape=jax.ShapeDtypeStruct((rows, dp * columns // mp), bf16),
        in_specs=[vmem] * 9 + [away] * 3,
        out_specs=vmem,
        scratch_shapes=[
            pltpu.VMEM(key_cache.shape, bf16),
            pltpu.VMEM(cached_values.shape, bf16),
            pltpu.VMEM(out_weight.shape, bf16),
            pltpu.VMEM((items, row_width), f32),
            pltpu.VMEM((dp, capacity, row_width), bf16),
            pltpu.VMEM((dp, capacity, row_width), bf16),
            pltpu.VMEM((slots, heads, kv_width), f32),
            pltpu.VMEM((3, slots, kv_width), f32),
            pltpu.VMEM((slots, key_cache.shape[1]), f32),
            pltpu.VMEM((slots, heads, HEAD_SIZE), f32),
            pltpu.VMEM((dp, slots, query_width), bf16),
            pltpu.VMEM((dp * rows, dp * slots), bf16),
            pltpu.VMEM((dp, rows, columns), bf16),
            pltpu.VMEM((dp, rows, columns), bf16),
            pltpu.SemaphoreType.DMA((3,)),
            pltpu.SemaphoreType.DMA((3, dp)),
            pltpu.SemaphoreType.DMA((3, dp)),
        ],
        compiler_params=pltpu.CompilerParams(
            collective_id=0, has_side_effects=True, vmem_limit_bytes=60 * 1024 * 1024
        ),
    )(
        queries,
        incoming_key,
        incoming_value,
        task_key_scale,
        task_value_scale,
        task_id.reshape(1, -1),
        cached_length.reshape(1, -1),
        cache_slot.reshape(1, -1),
        task_owner.reshape(1, -1),
        key_cache,
        cached_values,
        out_weight,
    )


def solution(mesh):
    placed = (
        P("dp", "mp"),
        P("dp", "mp"),
        P("dp", "mp"),
        P("dp", None, "mp"),
        P("dp", None, "mp"),
        P(None, "mp"),
        P(None, "mp"),
        P("mp", "dp"),
        P("dp"),
        P("dp"),
        P(),
        P("dp"),
    )
    return jax.shard_map(
        functools.partial(on_device, mesh.shape["dp"], mesh.shape["mp"]),
        mesh=mesh,
        in_specs=placed,
        out_specs=P("dp", "mp"),
        check_vma=False,
    )
```

```python
import functools
import math

import jax
import jax.numpy as jnp
from jax import lax
from jax.experimental import pallas as pl
from jax.experimental.pallas import tpu as pltpu
from jax.sharding import PartitionSpec as P

KEY_VALUE_HEADS = 8
HEAD_SIZE = 128
QUERY_HEADS = 64
GROUP = QUERY_HEADS // KEY_VALUE_HEADS
META = 128
FIRST = 16
CHUNKS = 4
MESH = pl.DeviceIdType.MESH

masked_score = -1e30
f32 = jnp.float32
bf16 = jnp.bfloat16


def iota(shape, dim):
    return lax.broadcasted_iota(jnp.int32, shape, dim)


def to_column(row):
    n = row.shape[1]
    eye = iota((n, n), 0) == iota((n, n), 1)
    return jnp.sum(jnp.where(eye, row, 0.0), axis=1, keepdims=True)


def to_row(column):
    n = column.shape[0]
    eye = iota((n, n), 0) == iota((n, n), 1)
    return jnp.sum(jnp.where(eye, column, 0.0), axis=0, keepdims=True)


def factors(dp):
    inner = 2 ** (int(math.log2(dp)) // 2)
    return dp // inner, inner


def dot(a, b):
    return jnp.dot(a, b, preferred_element_type=f32)


def layer_kernel(
    dp,
    mp,
    query_ref,
    new_key_ref,
    new_value_ref,
    key_scale_ref,
    value_scale_ref,
    task_ref,
    length_ref,
    slot_ref,
    owner_ref,
    key_hbm,
    value_hbm,
    weight_hbm,
    out_ref,
    keys,
    values,
    weight,
    rows_f32,
    send_rows,
    recv_rows,
    slot_query,
    slot_small,
    slot_length,
    slot_context,
    context,
    selector,
    send_part,
    recv_part,
    local_sem,
    send_sem,
    recv_sem,
    along_send,
    along_recv,
    across_send,
    across_recv,
):
    me = lax.axis_index("dp")
    part = lax.axis_index("mp")
    rows, query_width = query_ref.shape
    kv_width = new_key_ref.shape[1]
    kv_heads = kv_width // HEAD_SIZE
    heads = kv_heads * GROUP
    task_total = key_scale_ref.shape[0]
    slots, positions, _ = keys.shape
    capacity = send_rows.shape[1]
    items = dp * capacity
    columns = weight.shape[1]
    blocks = dp // mp
    meta_at = query_width + 2 * kv_width
    chunks, chunk = context.shape[1:3]
    outer, inner = factors(dp)

    total = dp * mp
    here = me * mp + part
    barrier = pltpu.get_barrier_semaphore()

    def greet(k, carry):
        other = lax.rem(here + k, total)
        pl.semaphore_signal(
            barrier,
            inc=1,
            device_id=(other // mp, lax.rem(other, mp)),
            device_id_type=MESH,
        )
        return carry

    lax.fori_loop(1, total, greet, 0)

    fetches = [
        pltpu.make_async_copy(key_hbm, keys, local_sem.at[0]),
        pltpu.make_async_copy(value_hbm, values, local_sem.at[1]),
        pltpu.make_async_copy(weight_hbm, weight, local_sem.at[2]),
    ]
    for fetch in fetches:
        fetch.start()

    task_column = to_column(task_ref[...].astype(f32))
    length_column = to_column(length_ref[...].astype(f32))
    slot_column = to_column(slot_ref[...].astype(f32))
    picked = task_column == iota((rows, task_total), 1).astype(f32)
    owner_column = jnp.sum(
        jnp.where(picked, owner_ref[...].astype(f32), 0.0), axis=1, keepdims=True
    )
    owner_row = to_row(owner_column)
    earlier = iota((rows, rows), 1) < iota((rows, rows), 0)
    rank = jnp.sum(
        jnp.where(earlier & (owner_column == owner_row), 1.0, 0.0), axis=1, keepdims=True
    )
    position_row = to_row(owner_column * capacity + rank)
    packer = jnp.where(position_row == iota((items, rows), 0).astype(f32), 1.0, 0.0).astype(bf16)
    key_factor = dot(jnp.where(picked, 1.0, 0.0).astype(bf16), key_scale_ref[...])
    for h in range(heads):
        g = h // GROUP
        lanes = slice(h * HEAD_SIZE, (h + 1) * HEAD_SIZE)
        scaled = (
            query_ref[:, lanes].astype(f32) * key_factor[:, g * HEAD_SIZE : (g + 1) * HEAD_SIZE]
        ).astype(bf16)
        rows_f32[:, lanes] = dot(packer, scaled)
    rows_f32[:, query_width : query_width + kv_width] = dot(packer, new_key_ref[...])
    rows_f32[:, query_width + kv_width : meta_at] = dot(packer, new_value_ref[...])
    lane = iota((rows, META), 1)
    line = iota((rows, META), 0)
    task_high = jnp.floor(task_column * (1.0 / 128.0))
    task_low = task_column - task_high * 128.0
    facts = (
        jnp.where(lane == 0, slot_column + 1.0, 0.0)
        + jnp.where(lane == 1, length_column, 0.0)
        + jnp.where(lane == 2, task_high, 0.0)
        + jnp.where(lane == 3, task_low, 0.0)
    )
    shared = jnp.sum(
        jnp.where(lane == FIRST + line, owner_column, 0.0)
        + jnp.where(lane == FIRST + rows + line, slot_column, 0.0),
        axis=0,
        keepdims=True,
    )
    rows_f32[:, meta_at:] = dot(packer, facts.astype(bf16)) + shared
    for d in range(dp):
        send_rows[d] = rows_f32[d * capacity : (d + 1) * capacity, :].astype(bf16)

    pl.semaphore_wait(barrier, total - 1)

    def request_copy(k):
        return pltpu.make_async_remote_copy(
            src_ref=send_rows.at[lax.rem(me + k, dp)],
            dst_ref=recv_rows.at[me],
            send_sem=send_sem.at[0, k],
            recv_sem=recv_sem.at[0, k],
            device_id=(lax.rem(me + k, dp), part),
            device_id_type=MESH,
        )

    def request_arrival(k):
        return pltpu.make_async_remote_copy(
            src_ref=send_rows.at[0],
            dst_ref=recv_rows.at[lax.rem(me + dp - k, dp)],
            send_sem=send_sem.at[0, k],
            recv_sem=recv_sem.at[0, k],
            device_id=(lax.rem(me + k, dp), part),
            device_id_type=MESH,
        )

    for k in range(1, dp):
        request_copy(k).start()
    recv_rows[me] = send_rows[me]
    slot_query[...] = jnp.zeros_like(slot_query)
    for k in range(1, dp):
        request_arrival(k).wait_recv()

    for s in range(dp):
        rows_f32[s * capacity : (s + 1) * capacity, :] = recv_rows[s].astype(f32)
    facts_in = rows_f32[:, meta_at:]
    placing_row = to_row(facts_in[:, 0:1])
    placer = jnp.where(
        placing_row == iota((slots, items), 0).astype(f32) + 1.0, 1.0, 0.0
    ).astype(bf16)
    for h in range(heads):
        g = h // GROUP
        slot_query[:, h, g * HEAD_SIZE : (g + 1) * HEAD_SIZE] = dot(
            placer, rows_f32[:, h * HEAD_SIZE : (h + 1) * HEAD_SIZE].astype(bf16)
        )
    slot_small[0] = dot(placer, rows_f32[:, query_width : query_width + kv_width].astype(bf16))
    slot_small[1] = dot(placer, rows_f32[:, query_width + kv_width : meta_at].astype(bf16))
    slot_facts = dot(placer, facts_in.astype(bf16))
    slot_task = slot_facts[:, 2:3] * 128.0 + slot_facts[:, 3:4]
    slot_small[2] = dot(
        jnp.where(slot_task == iota((slots, task_total), 1).astype(f32), 1.0, 0.0).astype(bf16),
        value_scale_ref[...],
    )
    slot_length[...] = jnp.broadcast_to(slot_facts[:, 1:2], (slots, positions))

    fetches[0].wait()
    fetches[1].wait()
    inv_root = 1.0 / math.sqrt(HEAD_SIZE)
    key_line = iota((heads, positions), 1).astype(f32)

    def attend(s, carry):
        query = slot_query[s]
        one = pl.ds(s, 1)
        fresh_key = slot_small[0, one, :]
        fresh_value = slot_small[1, one, :]
        value_factor = slot_small[2, one, :]
        length = slot_length[one, :]
        scores = (
            lax.dot_general(
                query.astype(bf16), keys[s], (((1,), (1,)), ((), ())), preferred_element_type=f32
            )
            * inv_root
        )
        own = jnp.sum(query * fresh_key, axis=1, keepdims=True) * inv_root
        visible = key_line < length
        scores = jnp.where(visible, scores, masked_score)
        top = jnp.maximum(jnp.max(scores, axis=1, keepdims=True), own)
        weights = jnp.where(visible, jnp.exp(scores - top), 0.0)
        own_weight = jnp.exp(own - top)
        weight_sum = jnp.sum(weights, axis=1, keepdims=True) + own_weight
        blended = dot(weights.astype(bf16), values[s])
        blended = blended + own_weight.astype(bf16).astype(f32) * fresh_value
        attended = (blended / weight_sum).astype(bf16).astype(f32) * value_factor
        for g in range(kv_heads):
            slot_context[s, g * GROUP : (g + 1) * GROUP, :] = attended[
                g * GROUP : (g + 1) * GROUP, g * HEAD_SIZE : (g + 1) * HEAD_SIZE
            ]
        return carry

    column, line_in = me // inner, lax.rem(me, inner)

    def source_of(k):
        return lax.rem(column + outer - k, outer) * inner + line_in

    def along_copy(k, c, source):
        return pltpu.make_async_remote_copy(
            src_ref=context.at[source, c],
            dst_ref=context.at[source, c],
            send_sem=along_send.at[k, c],
            recv_sem=along_recv.at[k, c],
            device_id=(lax.rem(column + k, outer) * inner + line_in, part),
            device_id_type=MESH,
        )

    def across_copy(k, j, c, source):
        return pltpu.make_async_remote_copy(
            src_ref=context.at[source, c],
            dst_ref=context.at[source, c],
            send_sem=across_send.at[k, j, c],
            recv_sem=across_recv.at[k, j, c],
            device_id=(column * inner + lax.rem(line_in + j, inner), part),
            device_id_type=MESH,
        )

    def forward(c):
        for k in range(1, outer):
            along_copy(k, c, source_of(k)).wait_recv()
            for j in range(1, inner):
                across_copy(k, j, c, source_of(k)).start()

    for c in range(chunks):
        lax.fori_loop(c * chunk, (c + 1) * chunk, attend, 0, unroll=min(chunk, 8))
        for h in range(heads):
            context[me, c, :, h * HEAD_SIZE : (h + 1) * HEAD_SIZE] = slot_context[
                c * chunk : (c + 1) * chunk, h, :
            ].astype(bf16)
        for k in range(outer - 1, 0, -1):
            along_copy(k, c, me).start()
        for j in range(1, inner):
            across_copy(0, j, c, me).start()
        if c > 0:
            forward(c - 1)

    lane_r = iota((rows, META), 1)
    line_r = iota((rows, META), 0)
    for s in range(dp):
        fact_row = rows_f32[s * capacity : s * capacity + 1, meta_at:]
        owner_in = jnp.sum(
            jnp.where(lane_r == FIRST + line_r, fact_row, 0.0), axis=1, keepdims=True
        )
        slot_in = jnp.sum(
            jnp.where(lane_r == FIRST + rows + line_r, fact_row, 0.0), axis=1, keepdims=True
        )
        selector[s * rows : (s + 1) * rows, :] = jnp.where(
            owner_in * slots + slot_in == iota((rows, dp * slots), 1).astype(f32), 1.0, 0.0
        ).astype(bf16)
    fetches[2].wait()
    forward(chunks - 1)
    for c in range(chunks):
        for k in range(outer):
            for j in range(1, inner):
                source = lax.rem(column + outer - k, outer) * inner + lax.rem(
                    line_in + inner - j, inner
                )
                across_copy(k, j, c, source).wait_recv()

    arranged = dot(selector[...], context[...].reshape(dp * slots, query_width)).astype(bf16)
    send_part[...] = dot(arranged, weight[...]).astype(bf16).reshape(dp, rows, columns)

    target_part = me // blocks
    place = lax.rem(me, blocks) * mp + part

    def part_copy(k):
        target = lax.rem(me + k, dp)
        return pltpu.make_async_remote_copy(
            src_ref=send_part.at[target],
            dst_ref=recv_part.at[place],
            send_sem=send_sem.at[2, k],
            recv_sem=recv_sem.at[2, place],
            device_id=(target, target_part),
            device_id_type=MESH,
        )

    def part_arrival(j):
        return pltpu.make_async_remote_copy(
            src_ref=send_part.at[0],
            dst_ref=recv_part.at[j],
            send_sem=send_sem.at[2, 0],
            recv_sem=recv_sem.at[2, j],
            device_id=(me, part),
            device_id_type=MESH,
        )

    for k in range(1, dp):
        part_copy(k).start()

    @pl.when(target_part != part)
    def _():
        part_copy(0).start()

    @pl.when(target_part == part)
    def _():
        recv_part[place] = send_part[me]

    for j in range(dp):
        own_block = (part * blocks + j // mp == me) & (part == j % mp)

        @pl.when(jnp.logical_not(own_block))
        def _():
            part_arrival(j).wait_recv()

    for e in range(blocks):
        summed = recv_part[e * mp].astype(f32)
        for j in range(1, mp):
            summed = summed + recv_part[e * mp + j].astype(f32)
        out_ref[:, e * columns : (e + 1) * columns] = summed.astype(bf16)

    for k in range(1, dp):
        request_copy(k).wait_send()
        part_copy(k).wait_send()

    for c in range(chunks):
        for k in range(outer):
            if k > 0:
                along_copy(k, c, me).wait_send()
            for j in range(1, inner):
                across_copy(k, j, c, source_of(k)).wait_send()

    @pl.when(target_part != part)
    def _():
        part_copy(0).wait_send()


def on_device(
    dp,
    mp,
    queries,
    incoming_key,
    incoming_value,
    key_cache,
    cached_values,
    task_key_scale,
    task_value_scale,
    out_weight,
    task_id,
    cached_length,
    task_owner,
    cache_slot,
):
    rows, query_width = queries.shape
    kv_width = incoming_key.shape[1]
    slots = key_cache.shape[0]
    capacity = 2 * rows // dp
    items = dp * capacity
    columns = out_weight.shape[1]
    row_width = query_width + 2 * kv_width + META
    heads = query_width // HEAD_SIZE
    outer, inner = factors(dp)
    vmem = pl.BlockSpec(memory_space=pltpu.VMEM)
    away = pl.BlockSpec(memory_space=pl.ANY)
    return pl.pallas_call(
        functools.partial(layer_kernel, dp, mp),
        out_shape=jax.ShapeDtypeStruct((rows, dp * columns // mp), bf16),
        in_specs=[vmem] * 9 + [away] * 3,
        out_specs=vmem,
        scratch_shapes=[
            pltpu.VMEM(key_cache.shape, bf16),
            pltpu.VMEM(cached_values.shape, bf16),
            pltpu.VMEM(out_weight.shape, bf16),
            pltpu.VMEM((items, row_width), f32),
            pltpu.VMEM((dp, capacity, row_width), bf16),
            pltpu.VMEM((dp, capacity, row_width), bf16),
            pltpu.VMEM((slots, heads, kv_width), f32),
            pltpu.VMEM((3, slots, kv_width), f32),
            pltpu.VMEM((slots, key_cache.shape[1]), f32),
            pltpu.VMEM((slots, heads, HEAD_SIZE), f32),
            pltpu.VMEM((dp, CHUNKS, slots // CHUNKS, query_width), bf16),
            pltpu.VMEM((dp * rows, dp * slots), bf16),
            pltpu.VMEM((dp, rows, columns), bf16),
            pltpu.VMEM((dp, rows, columns), bf16),
            pltpu.SemaphoreType.DMA((3,)),
            pltpu.SemaphoreType.DMA((3, dp)),
            pltpu.SemaphoreType.DMA((3, dp)),
            pltpu.SemaphoreType.DMA((outer, CHUNKS)),
            pltpu.SemaphoreType.DMA((outer, CHUNKS)),
            pltpu.SemaphoreType.DMA((outer, inner, CHUNKS)),
            pltpu.SemaphoreType.DMA((outer, inner, CHUNKS)),
        ],
        compiler_params=pltpu.CompilerParams(
            collective_id=0, has_side_effects=True, vmem_limit_bytes=60 * 1024 * 1024
        ),
    )(
        queries,
        incoming_key,
        incoming_value,
        task_key_scale,
        task_value_scale,
        task_id.reshape(1, -1),
        cached_length.reshape(1, -1),
        cache_slot.reshape(1, -1),
        task_owner.reshape(1, -1),
        key_cache,
        cached_values,
        out_weight,
    )


def solution(mesh):
    placed = (
        P("dp", "mp"),
        P("dp", "mp"),
        P("dp", "mp"),
        P("dp", None, "mp"),
        P("dp", None, "mp"),
        P(None, "mp"),
        P(None, "mp"),
        P("mp", "dp"),
        P("dp"),
        P("dp"),
        P(),
        P("dp"),
    )
    return jax.shard_map(
        functools.partial(on_device, mesh.shape["dp"], mesh.shape["mp"]),
        mesh=mesh,
        in_specs=placed,
        out_specs=P("dp", "mp"),
        check_vma=False,
    )
```

```python
import functools
import math

import jax
import jax.numpy as jnp
from jax import lax
from jax.experimental import pallas as pl
from jax.experimental.pallas import tpu as pltpu
from jax.sharding import PartitionSpec as P

KEY_VALUE_HEADS = 8
HEAD_SIZE = 128
QUERY_HEADS = 64
GROUP = QUERY_HEADS // KEY_VALUE_HEADS
META = 128
FIRST = 16
TOGETHER = 8
CHUNKS = 4
MESH = pl.DeviceIdType.MESH

masked_score = -1e30
f32 = jnp.float32
bf16 = jnp.bfloat16


def iota(shape, dim):
    return lax.broadcasted_iota(jnp.int32, shape, dim)


def to_column(row):
    n = row.shape[1]
    eye = iota((n, n), 0) == iota((n, n), 1)
    return jnp.sum(jnp.where(eye, row, 0.0), axis=1, keepdims=True)


def to_row(column):
    n = column.shape[0]
    eye = iota((n, n), 0) == iota((n, n), 1)
    return jnp.sum(jnp.where(eye, column, 0.0), axis=0, keepdims=True)


def factors(dp):
    inner = 2 ** (int(math.log2(dp)) // 2)
    return dp // inner, inner


def dot(a, b):
    return jnp.dot(a, b, preferred_element_type=f32)


def layer_kernel(
    dp,
    mp,
    query_ref,
    new_key_ref,
    new_value_ref,
    key_scale_ref,
    value_scale_ref,
    task_ref,
    length_ref,
    slot_ref,
    owner_ref,
    key_hbm,
    value_hbm,
    weight_hbm,
    out_ref,
    keys,
    values,
    weight,
    rows_f32,
    send_rows,
    recv_rows,
    slot_query,
    slot_small,
    slot_length,
    slot_context,
    context,
    selector,
    send_part,
    recv_part,
    local_sem,
    send_sem,
    recv_sem,
    along_send,
    along_recv,
    across_send,
    across_recv,
):
    me = lax.axis_index("dp")
    part = lax.axis_index("mp")
    rows, query_width = query_ref.shape
    kv_width = new_key_ref.shape[1]
    kv_heads = kv_width // HEAD_SIZE
    heads = kv_heads * GROUP
    task_total = key_scale_ref.shape[0]
    slots, positions, _ = keys.shape
    capacity = send_rows.shape[1]
    items = dp * capacity
    columns = weight.shape[1]
    blocks = dp // mp
    meta_at = query_width + 2 * kv_width
    chunks, chunk = context.shape[1:3]
    outer, inner = factors(dp)

    total = dp * mp
    here = me * mp + part
    barrier = pltpu.get_barrier_semaphore()

    def greet(k, carry):
        other = lax.rem(here + k, total)
        pl.semaphore_signal(
            barrier,
            inc=1,
            device_id=(other // mp, lax.rem(other, mp)),
            device_id_type=MESH,
        )
        return carry

    lax.fori_loop(1, total, greet, 0)

    fetches = [
        pltpu.make_async_copy(key_hbm, keys, local_sem.at[0]),
        pltpu.make_async_copy(value_hbm, values, local_sem.at[1]),
        pltpu.make_async_copy(weight_hbm, weight, local_sem.at[2]),
    ]
    for fetch in fetches:
        fetch.start()

    task_column = to_column(task_ref[...].astype(f32))
    length_column = to_column(length_ref[...].astype(f32))
    slot_column = to_column(slot_ref[...].astype(f32))
    picked = task_column == iota((rows, task_total), 1).astype(f32)
    owner_column = jnp.sum(
        jnp.where(picked, owner_ref[...].astype(f32), 0.0), axis=1, keepdims=True
    )
    owner_row = to_row(owner_column)
    earlier = iota((rows, rows), 1) < iota((rows, rows), 0)
    rank = jnp.sum(
        jnp.where(earlier & (owner_column == owner_row), 1.0, 0.0), axis=1, keepdims=True
    )
    position_row = to_row(owner_column * capacity + rank)
    packer = jnp.where(position_row == iota((items, rows), 0).astype(f32), 1.0, 0.0).astype(bf16)
    key_factor = dot(jnp.where(picked, 1.0, 0.0).astype(bf16), key_scale_ref[...])
    for h in range(heads):
        g = h // GROUP
        lanes = slice(h * HEAD_SIZE, (h + 1) * HEAD_SIZE)
        scaled = (
            query_ref[:, lanes].astype(f32) * key_factor[:, g * HEAD_SIZE : (g + 1) * HEAD_SIZE]
        ).astype(bf16)
        rows_f32[:, lanes] = dot(packer, scaled)
    rows_f32[:, query_width : query_width + kv_width] = dot(packer, new_key_ref[...])
    rows_f32[:, query_width + kv_width : meta_at] = dot(packer, new_value_ref[...])
    lane = iota((rows, META), 1)
    line = iota((rows, META), 0)
    task_high = jnp.floor(task_column * (1.0 / 128.0))
    task_low = task_column - task_high * 128.0
    facts = (
        jnp.where(lane == 0, slot_column + 1.0, 0.0)
        + jnp.where(lane == 1, length_column, 0.0)
        + jnp.where(lane == 2, task_high, 0.0)
        + jnp.where(lane == 3, task_low, 0.0)
    )
    shared = jnp.sum(
        jnp.where(lane == FIRST + line, owner_column, 0.0)
        + jnp.where(lane == FIRST + rows + line, slot_column, 0.0),
        axis=0,
        keepdims=True,
    )
    rows_f32[:, meta_at:] = dot(packer, facts.astype(bf16)) + shared
    for d in range(dp):
        send_rows[d] = rows_f32[d * capacity : (d + 1) * capacity, :].astype(bf16)

    pl.semaphore_wait(barrier, total - 1)

    def request_copy(k):
        return pltpu.make_async_remote_copy(
            src_ref=send_rows.at[lax.rem(me + k, dp)],
            dst_ref=recv_rows.at[me],
            send_sem=send_sem.at[0, k],
            recv_sem=recv_sem.at[0, k],
            device_id=(lax.rem(me + k, dp), part),
            device_id_type=MESH,
        )

    def request_arrival(k):
        return pltpu.make_async_remote_copy(
            src_ref=send_rows.at[0],
            dst_ref=recv_rows.at[lax.rem(me + dp - k, dp)],
            send_sem=send_sem.at[0, k],
            recv_sem=recv_sem.at[0, k],
            device_id=(lax.rem(me + k, dp), part),
            device_id_type=MESH,
        )

    for k in range(1, dp):
        request_copy(k).start()
    recv_rows[me] = send_rows[me]
    slot_query[...] = jnp.zeros_like(slot_query)
    for k in range(1, dp):
        request_arrival(k).wait_recv()

    for s in range(dp):
        rows_f32[s * capacity : (s + 1) * capacity, :] = recv_rows[s].astype(f32)
    facts_in = rows_f32[:, meta_at:]
    placing_row = to_row(facts_in[:, 0:1])
    placer = jnp.where(
        placing_row == iota((slots, items), 0).astype(f32) + 1.0, 1.0, 0.0
    ).astype(bf16)
    for h in range(heads):
        g = h // GROUP
        slot_query[:, h, g * HEAD_SIZE : (g + 1) * HEAD_SIZE] = dot(
            placer, rows_f32[:, h * HEAD_SIZE : (h + 1) * HEAD_SIZE].astype(bf16)
        )
    slot_small[0] = dot(placer, rows_f32[:, query_width : query_width + kv_width].astype(bf16))
    slot_small[1] = dot(placer, rows_f32[:, query_width + kv_width : meta_at].astype(bf16))
    slot_facts = dot(placer, facts_in.astype(bf16))
    slot_task = slot_facts[:, 2:3] * 128.0 + slot_facts[:, 3:4]
    slot_small[2] = dot(
        jnp.where(slot_task == iota((slots, task_total), 1).astype(f32), 1.0, 0.0).astype(bf16),
        value_scale_ref[...],
    )
    slot_length[...] = jnp.broadcast_to(slot_facts[:, 1:2], (slots, positions))

    fetches[0].wait()
    fetches[1].wait()
    inv_root = 1.0 / math.sqrt(HEAD_SIZE)
    key_line = iota((heads, positions), 1).astype(f32)

    def attend(n, carry):
        picks = [n * TOGETHER + i for i in range(TOGETHER)]
        scores, owns, weights, own_weights, sums, tops = [], [], [], [], [], []
        for s in picks:
            scores.append(
                lax.dot_general(
                    slot_query[s].astype(bf16),
                    keys[s],
                    (((1,), (1,)), ((), ())),
                    preferred_element_type=f32,
                )
                * inv_root
            )
        for s in picks:
            owns.append(
                jnp.sum(slot_query[s] * slot_small[0, pl.ds(s, 1), :], axis=1, keepdims=True)
                * inv_root
            )
        for i, s in enumerate(picks):
            visible = key_line < slot_length[pl.ds(s, 1), :]
            shown = jnp.where(visible, scores[i], masked_score)
            tops.append(jnp.maximum(jnp.max(shown, axis=1, keepdims=True), owns[i]))
        for i, s in enumerate(picks):
            visible = key_line < slot_length[pl.ds(s, 1), :]
            shown = jnp.where(visible, scores[i], masked_score)
            weights.append(jnp.where(visible, jnp.exp(shown - tops[i]), 0.0))
            own_weights.append(jnp.exp(owns[i] - tops[i]))
        blends = [dot(weights[i].astype(bf16), values[s]) for i, s in enumerate(picks)]
        for i in range(TOGETHER):
            sums.append(jnp.sum(weights[i], axis=1, keepdims=True) + own_weights[i])
        for i, s in enumerate(picks):
            one = pl.ds(s, 1)
            blended = blends[i] + own_weights[i].astype(bf16).astype(f32) * slot_small[1, one, :]
            attended = (blended / sums[i]).astype(bf16).astype(f32) * slot_small[2, one, :]
            for g in range(kv_heads):
                slot_context[s, g * GROUP : (g + 1) * GROUP, :] = attended[
                    g * GROUP : (g + 1) * GROUP, g * HEAD_SIZE : (g + 1) * HEAD_SIZE
                ]
        return carry

    column, line_in = me // inner, lax.rem(me, inner)

    def source_of(k):
        return lax.rem(column + outer - k, outer) * inner + line_in

    def along_copy(k, c, source):
        return pltpu.make_async_remote_copy(
            src_ref=context.at[source, c],
            dst_ref=context.at[source, c],
            send_sem=along_send.at[k, c],
            recv_sem=along_recv.at[k, c],
            device_id=(lax.rem(column + k, outer) * inner + line_in, part),
            device_id_type=MESH,
        )

    def across_copy(k, j, c, source):
        return pltpu.make_async_remote_copy(
            src_ref=context.at[source, c],
            dst_ref=context.at[source, c],
            send_sem=across_send.at[k, j, c],
            recv_sem=across_recv.at[k, j, c],
            device_id=(column * inner + lax.rem(line_in + j, inner), part),
            device_id_type=MESH,
        )

    def forward(c):
        for k in range(1, outer):
            along_copy(k, c, source_of(k)).wait_recv()
            for j in range(1, inner):
                across_copy(k, j, c, source_of(k)).start()

    for c in range(chunks):
        lax.fori_loop(c * chunk // TOGETHER, (c + 1) * chunk // TOGETHER, attend, 0)
        for h in range(heads):
            context[me, c, :, h * HEAD_SIZE : (h + 1) * HEAD_SIZE] = slot_context[
                c * chunk : (c + 1) * chunk, h, :
            ].astype(bf16)
        for k in range(outer - 1, 0, -1):
            along_copy(k, c, me).start()
        for j in range(1, inner):
            across_copy(0, j, c, me).start()
        if c > 0:
            forward(c - 1)

    lane_r = iota((rows, META), 1)
    line_r = iota((rows, META), 0)
    for s in range(dp):
        fact_row = rows_f32[s * capacity : s * capacity + 1, meta_at:]
        owner_in = jnp.sum(
            jnp.where(lane_r == FIRST + line_r, fact_row, 0.0), axis=1, keepdims=True
        )
        slot_in = jnp.sum(
            jnp.where(lane_r == FIRST + rows + line_r, fact_row, 0.0), axis=1, keepdims=True
        )
        selector[s * rows : (s + 1) * rows, :] = jnp.where(
            owner_in * slots + slot_in == iota((rows, dp * slots), 1).astype(f32), 1.0, 0.0
        ).astype(bf16)
    fetches[2].wait()
    forward(chunks - 1)
    for c in range(chunks):
        for k in range(outer):
            for j in range(1, inner):
                source = lax.rem(column + outer - k, outer) * inner + lax.rem(
                    line_in + inner - j, inner
                )
                across_copy(k, j, c, source).wait_recv()

    arranged = dot(selector[...], context[...].reshape(dp * slots, query_width)).astype(bf16)
    send_part[...] = dot(arranged, weight[...]).astype(bf16).reshape(dp, rows, columns)

    target_part = me // blocks
    place = lax.rem(me, blocks) * mp + part

    def part_copy(k):
        target = lax.rem(me + k, dp)
        return pltpu.make_async_remote_copy(
            src_ref=send_part.at[target],
            dst_ref=recv_part.at[place],
            send_sem=send_sem.at[2, k],
            recv_sem=recv_sem.at[2, place],
            device_id=(target, target_part),
            device_id_type=MESH,
        )

    def part_arrival(j):
        return pltpu.make_async_remote_copy(
            src_ref=send_part.at[0],
            dst_ref=recv_part.at[j],
            send_sem=send_sem.at[2, 0],
            recv_sem=recv_sem.at[2, j],
            device_id=(me, part),
            device_id_type=MESH,
        )

    for k in range(1, dp):
        part_copy(k).start()

    @pl.when(target_part != part)
    def _():
        part_copy(0).start()

    @pl.when(target_part == part)
    def _():
        recv_part[place] = send_part[me]

    for j in range(dp):
        own_block = (part * blocks + j // mp == me) & (part == j % mp)

        @pl.when(jnp.logical_not(own_block))
        def _():
            part_arrival(j).wait_recv()

    for e in range(blocks):
        summed = recv_part[e * mp].astype(f32)
        for j in range(1, mp):
            summed = summed + recv_part[e * mp + j].astype(f32)
        out_ref[:, e * columns : (e + 1) * columns] = summed.astype(bf16)

    for k in range(1, dp):
        request_copy(k).wait_send()
        part_copy(k).wait_send()

    for c in range(chunks):
        for k in range(outer):
            if k > 0:
                along_copy(k, c, me).wait_send()
            for j in range(1, inner):
                across_copy(k, j, c, source_of(k)).wait_send()

    @pl.when(target_part != part)
    def _():
        part_copy(0).wait_send()


def on_device(
    dp,
    mp,
    queries,
    incoming_key,
    incoming_value,
    key_cache,
    cached_values,
    task_key_scale,
    task_value_scale,
    out_weight,
    task_id,
    cached_length,
    task_owner,
    cache_slot,
):
    rows, query_width = queries.shape
    kv_width = incoming_key.shape[1]
    slots = key_cache.shape[0]
    capacity = 2 * rows // dp
    items = dp * capacity
    columns = out_weight.shape[1]
    row_width = query_width + 2 * kv_width + META
    heads = query_width // HEAD_SIZE
    outer, inner = factors(dp)
    vmem = pl.BlockSpec(memory_space=pltpu.VMEM)
    away = pl.BlockSpec(memory_space=pl.ANY)
    return pl.pallas_call(
        functools.partial(layer_kernel, dp, mp),
        out_shape=jax.ShapeDtypeStruct((rows, dp * columns // mp), bf16),
        in_specs=[vmem] * 9 + [away] * 3,
        out_specs=vmem,
        scratch_shapes=[
            pltpu.VMEM(key_cache.shape, bf16),
            pltpu.VMEM(cached_values.shape, bf16),
            pltpu.VMEM(out_weight.shape, bf16),
            pltpu.VMEM((items, row_width), f32),
            pltpu.VMEM((dp, capacity, row_width), bf16),
            pltpu.VMEM((dp, capacity, row_width), bf16),
            pltpu.VMEM((slots, heads, kv_width), f32),
            pltpu.VMEM((3, slots, kv_width), f32),
            pltpu.VMEM((slots, key_cache.shape[1]), f32),
            pltpu.VMEM((slots, heads, HEAD_SIZE), f32),
            pltpu.VMEM((dp, CHUNKS, slots // CHUNKS, query_width), bf16),
            pltpu.VMEM((dp * rows, dp * slots), bf16),
            pltpu.VMEM((dp, rows, columns), bf16),
            pltpu.VMEM((dp, rows, columns), bf16),
            pltpu.SemaphoreType.DMA((3,)),
            pltpu.SemaphoreType.DMA((3, dp)),
            pltpu.SemaphoreType.DMA((3, dp)),
            pltpu.SemaphoreType.DMA((outer, CHUNKS)),
            pltpu.SemaphoreType.DMA((outer, CHUNKS)),
            pltpu.SemaphoreType.DMA((outer, inner, CHUNKS)),
            pltpu.SemaphoreType.DMA((outer, inner, CHUNKS)),
        ],
        compiler_params=pltpu.CompilerParams(
            collective_id=0, has_side_effects=True, vmem_limit_bytes=60 * 1024 * 1024
        ),
    )(
        queries,
        incoming_key,
        incoming_value,
        task_key_scale,
        task_value_scale,
        task_id.reshape(1, -1),
        cached_length.reshape(1, -1),
        cache_slot.reshape(1, -1),
        task_owner.reshape(1, -1),
        key_cache,
        cached_values,
        out_weight,
    )


def solution(mesh):
    placed = (
        P("dp", "mp"),
        P("dp", "mp"),
        P("dp", "mp"),
        P("dp", None, "mp"),
        P("dp", None, "mp"),
        P(None, "mp"),
        P(None, "mp"),
        P("mp", "dp"),
        P("dp"),
        P("dp"),
        P(),
        P("dp"),
    )
    return jax.shard_map(
        functools.partial(on_device, mesh.shape["dp"], mesh.shape["mp"]),
        mesh=mesh,
        in_specs=placed,
        out_specs=P("dp", "mp"),
        check_vma=False,
    )
```

```python
import functools
import math

import jax
import jax.numpy as jnp
from jax import lax
from jax.experimental import pallas as pl
from jax.experimental.pallas import tpu as pltpu
from jax.sharding import PartitionSpec as P

KEY_VALUE_HEADS = 8
HEAD_SIZE = 128
QUERY_HEADS = 64
GROUP = QUERY_HEADS // KEY_VALUE_HEADS
META = 128
FIRST = 16
TOGETHER = 8
CHUNKS = 4
MESH = pl.DeviceIdType.MESH

masked_score = -1e30
f32 = jnp.float32
bf16 = jnp.bfloat16


def iota(shape, dim):
    return lax.broadcasted_iota(jnp.int32, shape, dim)


def to_column(row):
    n = row.shape[1]
    eye = iota((n, n), 0) == iota((n, n), 1)
    return jnp.sum(jnp.where(eye, row, 0.0), axis=1, keepdims=True)


def to_row(column):
    n = column.shape[0]
    eye = iota((n, n), 0) == iota((n, n), 1)
    return jnp.sum(jnp.where(eye, column, 0.0), axis=0, keepdims=True)


def factors(dp):
    inner = 2 ** (int(math.log2(dp)) // 2)
    return dp // inner, inner


def dot(a, b):
    return jnp.dot(a, b, preferred_element_type=f32)


def layer_kernel(
    dp,
    mp,
    query_ref,
    new_key_ref,
    new_value_ref,
    key_scale_ref,
    value_scale_ref,
    task_ref,
    length_ref,
    slot_ref,
    owner_ref,
    key_hbm,
    value_hbm,
    weight_hbm,
    out_ref,
    keys,
    values,
    weight,
    rows_f32,
    send_rows,
    recv_rows,
    slot_query,
    slot_small,
    slot_length,
    slot_context,
    context,
    selector,
    send_part,
    recv_part,
    local_sem,
    send_sem,
    recv_sem,
    along_send,
    along_recv,
    across_send,
    across_recv,
):
    me = lax.axis_index("dp")
    part = lax.axis_index("mp")
    rows, query_width = query_ref.shape
    kv_width = new_key_ref.shape[1]
    kv_heads = kv_width // HEAD_SIZE
    heads = kv_heads * GROUP
    task_total = key_scale_ref.shape[0]
    slots, positions, _ = keys.shape
    capacity = send_rows.shape[1]
    items = dp * capacity
    columns = weight.shape[1]
    blocks = dp // mp
    meta_at = query_width + 2 * kv_width
    chunks, chunk = context.shape[1:3]
    outer, inner = factors(dp)

    total = dp * mp
    here = me * mp + part
    barrier = pltpu.get_barrier_semaphore()

    def greet(k, carry):
        other = lax.rem(here + k, total)
        pl.semaphore_signal(
            barrier,
            inc=1,
            device_id=(other // mp, lax.rem(other, mp)),
            device_id_type=MESH,
        )
        return carry

    lax.fori_loop(1, total, greet, 0)

    fetches = [
        pltpu.make_async_copy(key_hbm, keys, local_sem.at[0]),
        pltpu.make_async_copy(value_hbm, values, local_sem.at[1]),
        pltpu.make_async_copy(weight_hbm, weight, local_sem.at[2]),
    ]
    for fetch in fetches:
        fetch.start()

    task_column = to_column(task_ref[...].astype(f32))
    length_column = to_column(length_ref[...].astype(f32))
    slot_column = to_column(slot_ref[...].astype(f32))
    picked = task_column == iota((rows, task_total), 1).astype(f32)
    owner_column = jnp.sum(
        jnp.where(picked, owner_ref[...].astype(f32), 0.0), axis=1, keepdims=True
    )
    owner_row = to_row(owner_column)
    earlier = iota((rows, rows), 1) < iota((rows, rows), 0)
    rank = jnp.sum(
        jnp.where(earlier & (owner_column == owner_row), 1.0, 0.0), axis=1, keepdims=True
    )
    position_row = to_row(owner_column * capacity + rank)
    packer = jnp.where(position_row == iota((items, rows), 0).astype(f32), 1.0, 0.0).astype(bf16)
    key_factor = dot(jnp.where(picked, 1.0, 0.0).astype(bf16), key_scale_ref[...])
    for h in range(heads):
        g = h // GROUP
        lanes = slice(h * HEAD_SIZE, (h + 1) * HEAD_SIZE)
        scaled = (
            query_ref[:, lanes].astype(f32) * key_factor[:, g * HEAD_SIZE : (g + 1) * HEAD_SIZE]
        ).astype(bf16)
        rows_f32[:, lanes] = dot(packer, scaled)
    rows_f32[:, query_width : query_width + kv_width] = dot(packer, new_key_ref[...])
    rows_f32[:, query_width + kv_width : meta_at] = dot(packer, new_value_ref[...])
    lane = iota((rows, META), 1)
    line = iota((rows, META), 0)
    task_high = jnp.floor(task_column * (1.0 / 128.0))
    task_low = task_column - task_high * 128.0
    facts = (
        jnp.where(lane == 0, slot_column + 1.0, 0.0)
        + jnp.where(lane == 1, length_column, 0.0)
        + jnp.where(lane == 2, task_high, 0.0)
        + jnp.where(lane == 3, task_low, 0.0)
    )
    shared = jnp.sum(
        jnp.where(lane == FIRST + line, owner_column, 0.0)
        + jnp.where(lane == FIRST + rows + line, slot_column, 0.0),
        axis=0,
        keepdims=True,
    )
    rows_f32[:, meta_at:] = dot(packer, facts.astype(bf16)) + shared
    for d in range(dp):
        send_rows[d] = rows_f32[d * capacity : (d + 1) * capacity, :].astype(bf16)

    pl.semaphore_wait(barrier, total - 1)

    def request_copy(k):
        return pltpu.make_async_remote_copy(
            src_ref=send_rows.at[lax.rem(me + k, dp)],
            dst_ref=recv_rows.at[me],
            send_sem=send_sem.at[0, k],
            recv_sem=recv_sem.at[0, k],
            device_id=(lax.rem(me + k, dp), part),
            device_id_type=MESH,
        )

    def request_arrival(k):
        return pltpu.make_async_remote_copy(
            src_ref=send_rows.at[0],
            dst_ref=recv_rows.at[lax.rem(me + dp - k, dp)],
            send_sem=send_sem.at[0, k],
            recv_sem=recv_sem.at[0, k],
            device_id=(lax.rem(me + k, dp), part),
            device_id_type=MESH,
        )

    for k in range(1, dp):
        request_copy(k).start()
    recv_rows[me] = send_rows[me]
    slot_query[...] = jnp.zeros_like(slot_query)
    for k in range(1, dp):
        request_arrival(k).wait_recv()

    for s in range(dp):
        rows_f32[s * capacity : (s + 1) * capacity, :] = recv_rows[s].astype(f32)
    facts_in = rows_f32[:, meta_at:]
    placing_row = to_row(facts_in[:, 0:1])
    placer = jnp.where(
        placing_row == iota((slots, items), 0).astype(f32) + 1.0, 1.0, 0.0
    ).astype(bf16)
    for h in range(heads):
        g = h // GROUP
        slot_query[:, h, g * HEAD_SIZE : (g + 1) * HEAD_SIZE] = dot(
            placer, rows_f32[:, h * HEAD_SIZE : (h + 1) * HEAD_SIZE].astype(bf16)
        )
    slot_small[0] = dot(placer, rows_f32[:, query_width : query_width + kv_width].astype(bf16))
    slot_small[1] = dot(placer, rows_f32[:, query_width + kv_width : meta_at].astype(bf16))
    slot_facts = dot(placer, facts_in.astype(bf16))
    slot_task = slot_facts[:, 2:3] * 128.0 + slot_facts[:, 3:4]
    slot_small[2] = dot(
        jnp.where(slot_task == iota((slots, task_total), 1).astype(f32), 1.0, 0.0).astype(bf16),
        value_scale_ref[...],
    )
    slot_length[...] = jnp.broadcast_to(slot_facts[:, 1:2], (slots, positions))

    fetches[0].wait()
    fetches[1].wait()
    inv_root = 1.0 / math.sqrt(HEAD_SIZE)
    key_line = iota((heads, positions), 1).astype(f32)

    def attend(n, carry):
        picks = [n * TOGETHER + i for i in range(TOGETHER)]
        scores, owns, weights, own_weights, sums, tops = [], [], [], [], [], []
        for s in picks:
            scores.append(
                lax.dot_general(
                    slot_query[s].astype(bf16),
                    keys[s],
                    (((1,), (1,)), ((), ())),
                    preferred_element_type=f32,
                )
                * inv_root
            )
        for s in picks:
            owns.append(
                jnp.sum(slot_query[s] * slot_small[0, pl.ds(s, 1), :], axis=1, keepdims=True)
                * inv_root
            )
        for i, s in enumerate(picks):
            visible = key_line < slot_length[pl.ds(s, 1), :]
            shown = jnp.where(visible, scores[i], masked_score)
            tops.append(jnp.maximum(jnp.max(shown, axis=1, keepdims=True), owns[i]))
        for i, s in enumerate(picks):
            visible = key_line < slot_length[pl.ds(s, 1), :]
            shown = jnp.where(visible, scores[i], masked_score)
            weights.append(jnp.where(visible, jnp.exp(shown - tops[i]), 0.0))
            own_weights.append(jnp.exp(owns[i] - tops[i]))
        blends = [dot(weights[i].astype(bf16), values[s]) for i, s in enumerate(picks)]
        for i in range(TOGETHER):
            sums.append(jnp.sum(weights[i], axis=1, keepdims=True) + own_weights[i])
        for i, s in enumerate(picks):
            one = pl.ds(s, 1)
            blended = blends[i] + own_weights[i].astype(bf16).astype(f32) * slot_small[1, one, :]
            attended = (blended / sums[i]).astype(bf16).astype(f32) * slot_small[2, one, :]
            for g in range(kv_heads):
                slot_context[s, g * GROUP : (g + 1) * GROUP, :] = attended[
                    g * GROUP : (g + 1) * GROUP, g * HEAD_SIZE : (g + 1) * HEAD_SIZE
                ]
        return carry

    column, line_in = me // inner, lax.rem(me, inner)

    def source_of(k):
        return lax.rem(column + outer - k, outer) * inner + line_in

    def along_copy(k, c, source):
        return pltpu.make_async_remote_copy(
            src_ref=context.at[source, c],
            dst_ref=context.at[source, c],
            send_sem=along_send.at[k, c],
            recv_sem=along_recv.at[k, c],
            device_id=(lax.rem(column + k, outer) * inner + line_in, part),
            device_id_type=MESH,
        )

    def across_copy(k, j, c, source):
        return pltpu.make_async_remote_copy(
            src_ref=context.at[source, c],
            dst_ref=context.at[source, c],
            send_sem=across_send.at[k, j, c],
            recv_sem=across_recv.at[k, j, c],
            device_id=(column * inner + lax.rem(line_in + j, inner), part),
            device_id_type=MESH,
        )

    def forward(c):
        for k in (outer - 1, *range(1, outer - 1)):
            along_copy(k, c, source_of(k)).wait_recv()
            for j in range(1, inner):
                across_copy(k, j, c, source_of(k)).start()

    for c in range(chunks):
        lax.fori_loop(c * chunk // TOGETHER, (c + 1) * chunk // TOGETHER, attend, 0)
        for h in range(heads):
            context[me, c, :, h * HEAD_SIZE : (h + 1) * HEAD_SIZE] = slot_context[
                c * chunk : (c + 1) * chunk, h, :
            ].astype(bf16)
        for k in range(1, outer):
            along_copy(k, c, me).start()
        for j in range(1, inner):
            across_copy(0, j, c, me).start()
        if c > 0:
            forward(c - 1)

    lane_r = iota((rows, META), 1)
    line_r = iota((rows, META), 0)
    for s in range(dp):
        fact_row = rows_f32[s * capacity : s * capacity + 1, meta_at:]
        owner_in = jnp.sum(
            jnp.where(lane_r == FIRST + line_r, fact_row, 0.0), axis=1, keepdims=True
        )
        slot_in = jnp.sum(
            jnp.where(lane_r == FIRST + rows + line_r, fact_row, 0.0), axis=1, keepdims=True
        )
        selector[s * rows : (s + 1) * rows, :] = jnp.where(
            owner_in * slots + slot_in == iota((rows, dp * slots), 1).astype(f32), 1.0, 0.0
        ).astype(bf16)
    fetches[2].wait()
    forward(chunks - 1)
    for c in range(chunks):
        for k in range(outer):
            for j in range(1, inner):
                source = lax.rem(column + outer - k, outer) * inner + lax.rem(
                    line_in + inner - j, inner
                )
                across_copy(k, j, c, source).wait_recv()

    arranged = dot(selector[...], context[...].reshape(dp * slots, query_width)).astype(bf16)
    send_part[...] = dot(arranged, weight[...]).astype(bf16).reshape(dp, rows, columns)

    target_part = me // blocks
    place = lax.rem(me, blocks) * mp + part

    def part_copy(k):
        target = lax.rem(me + k, dp)
        return pltpu.make_async_remote_copy(
            src_ref=send_part.at[target],
            dst_ref=recv_part.at[place],
            send_sem=send_sem.at[2, k],
            recv_sem=recv_sem.at[2, place],
            device_id=(target, target_part),
            device_id_type=MESH,
        )

    def part_arrival(j):
        return pltpu.make_async_remote_copy(
            src_ref=send_part.at[0],
            dst_ref=recv_part.at[j],
            send_sem=send_sem.at[2, 0],
            recv_sem=recv_sem.at[2, j],
            device_id=(me, part),
            device_id_type=MESH,
        )

    for k in range(1, dp):
        part_copy(k).start()

    @pl.when(target_part != part)
    def _():
        part_copy(0).start()

    @pl.when(target_part == part)
    def _():
        recv_part[place] = send_part[me]

    for j in range(dp):
        own_block = (part * blocks + j // mp == me) & (part == j % mp)

        @pl.when(jnp.logical_not(own_block))
        def _():
            part_arrival(j).wait_recv()

    for e in range(blocks):
        summed = recv_part[e * mp].astype(f32)
        for j in range(1, mp):
            summed = summed + recv_part[e * mp + j].astype(f32)
        out_ref[:, e * columns : (e + 1) * columns] = summed.astype(bf16)

    for k in range(1, dp):
        request_copy(k).wait_send()
        part_copy(k).wait_send()

    for c in range(chunks):
        for k in range(outer):
            if k > 0:
                along_copy(k, c, me).wait_send()
            for j in range(1, inner):
                across_copy(k, j, c, source_of(k)).wait_send()

    @pl.when(target_part != part)
    def _():
        part_copy(0).wait_send()


def on_device(
    dp,
    mp,
    queries,
    incoming_key,
    incoming_value,
    key_cache,
    cached_values,
    task_key_scale,
    task_value_scale,
    out_weight,
    task_id,
    cached_length,
    task_owner,
    cache_slot,
):
    rows, query_width = queries.shape
    kv_width = incoming_key.shape[1]
    slots = key_cache.shape[0]
    capacity = 2 * rows // dp
    items = dp * capacity
    columns = out_weight.shape[1]
    row_width = query_width + 2 * kv_width + META
    heads = query_width // HEAD_SIZE
    outer, inner = factors(dp)
    vmem = pl.BlockSpec(memory_space=pltpu.VMEM)
    away = pl.BlockSpec(memory_space=pl.ANY)
    return pl.pallas_call(
        functools.partial(layer_kernel, dp, mp),
        out_shape=jax.ShapeDtypeStruct((rows, dp * columns // mp), bf16),
        in_specs=[vmem] * 9 + [away] * 3,
        out_specs=vmem,
        scratch_shapes=[
            pltpu.VMEM(key_cache.shape, bf16),
            pltpu.VMEM(cached_values.shape, bf16),
            pltpu.VMEM(out_weight.shape, bf16),
            pltpu.VMEM((items, row_width), f32),
            pltpu.VMEM((dp, capacity, row_width), bf16),
            pltpu.VMEM((dp, capacity, row_width), bf16),
            pltpu.VMEM((slots, heads, kv_width), f32),
            pltpu.VMEM((3, slots, kv_width), f32),
            pltpu.VMEM((slots, key_cache.shape[1]), f32),
            pltpu.VMEM((slots, heads, HEAD_SIZE), f32),
            pltpu.VMEM((dp, CHUNKS, slots // CHUNKS, query_width), bf16),
            pltpu.VMEM((dp * rows, dp * slots), bf16),
            pltpu.VMEM((dp, rows, columns), bf16),
            pltpu.VMEM((dp, rows, columns), bf16),
            pltpu.SemaphoreType.DMA((3,)),
            pltpu.SemaphoreType.DMA((3, dp)),
            pltpu.SemaphoreType.DMA((3, dp)),
            pltpu.SemaphoreType.DMA((outer, CHUNKS)),
            pltpu.SemaphoreType.DMA((outer, CHUNKS)),
            pltpu.SemaphoreType.DMA((outer, inner, CHUNKS)),
            pltpu.SemaphoreType.DMA((outer, inner, CHUNKS)),
        ],
        compiler_params=pltpu.CompilerParams(
            collective_id=0, has_side_effects=True, vmem_limit_bytes=60 * 1024 * 1024
        ),
    )(
        queries,
        incoming_key,
        incoming_value,
        task_key_scale,
        task_value_scale,
        task_id.reshape(1, -1),
        cached_length.reshape(1, -1),
        cache_slot.reshape(1, -1),
        task_owner.reshape(1, -1),
        key_cache,
        cached_values,
        out_weight,
    )


def solution(mesh):
    placed = (
        P("dp", "mp"),
        P("dp", "mp"),
        P("dp", "mp"),
        P("dp", None, "mp"),
        P("dp", None, "mp"),
        P(None, "mp"),
        P(None, "mp"),
        P("mp", "dp"),
        P("dp"),
        P("dp"),
        P(),
        P("dp"),
    )
    return jax.shard_map(
        functools.partial(on_device, mesh.shape["dp"], mesh.shape["mp"]),
        mesh=mesh,
        in_specs=placed,
        out_specs=P("dp", "mp"),
        check_vma=False,
    )
```
